128 devices in a mesh: grid: 32 (over x, z, core), orb: 4 (over y).
Axes of the slice: x: 4, y: 4, z: 4, core: 2. Of those that a mesh axis runs over, the one named last changes fastest.
Arguments:
- orbitals: bfloat16 [1800, 262144], P('orb', 'grid'), may hold values from -0.5 to 1.5
- pivots: int32 [3, 96], replicated, may hold values from 0 to 262143, as said below
Outputs:
- cholesky_factor: float32 [262144, 288], P(('grid', 'orb'))
- residual_diagonal: float32 [262144], P(('grid', 'orb'))
- diagonal_peaks: float32 [3], replicated
The draws below stay inside these ranges and needn't reach their ends.
Inputs may be any that keep to these rules, and one draw needn't show every extreme that they name: `pivots`: all 3 x 96 pivot indices are distinct grid points.
All inputs are finite; a program needn't handle non-finite values.
Results may differ from the reference program's by a relative error of at most 0.0003.
Values may be sent and summed in bfloat16 or wider, within the bound.
No kernel may reach another device: no remote copies, remote signals or barrier semaphores. Data moves between devices by JAX's collectives and lax.ppermute only.
A program may use at most 64 MiB of HBM per device.

```python
import jax
import jax.numpy as jnp
from jax import lax

ORB = 1800
PIV = 96
STEPS = 3
GRID_POINTS = 262144


def draw_pivots(key, part):
    order = jax.random.permutation(jax.random.fold_in(key, 11), GRID_POINTS)
    return order[:STEPS * PIV].reshape(STEPS, PIV).astype(jnp.int32)


def levels(stream_key, shape, pieces, smallest, largest):
    def one(axis_at, parts):
        draws = jax.random.uniform(jax.random.fold_in(jax.random.fold_in(stream_key, 6), axis_at), (parts,), jnp.float32, smallest / len(pieces), largest / len(pieces))
        return jnp.repeat(jnp.exp(draws), shape[axis_at] // parts).reshape((-1,) + (1,) * (len(shape) - axis_at - 1))

    loudness = one(*pieces[0])
    for cut in pieces[1:]:
        loudness = loudness * one(*cut)
    return loudness


def setup_inputs(seed: int = 0) -> dict:
    keys = jax.random.split(jax.random.key(seed), 3)
    orbitals = jnp.clip(-0.5 + 2.0 * jax.random.uniform(keys[0], (ORB, GRID_POINTS), jnp.float32) ** levels(keys[0], (ORB, GRID_POINTS), ((0, 4), (1, 32)), -0.2, 0.2), -0.5, 1.5).astype(jnp.bfloat16)
    pivots = draw_pivots(jax.random.fold_in(keys[2], 71), 0)
    return dict(orbitals=orbitals, pivots=pivots)


def reference(orbitals, pivots):
    grid_count = orbitals.shape[1]
    squares = jnp.sum(jnp.square(orbitals.astype(jnp.float32)), axis=0)
    diagonal = jnp.square(squares / ORB)
    factor = jnp.zeros((grid_count, STEPS * PIV), jnp.float32)
    peaks = []
    for section in range(STEPS):
        chosen = pivots[section]
        sampled = jnp.take(orbitals, chosen, axis=1)
        known = jnp.take(factor, chosen, axis=0)
        pair = lax.dot_general(sampled.astype(jnp.float32), sampled.astype(jnp.float32), (((0,), (0,)), ((), ())), preferred_element_type=jnp.float32)
        block = jnp.square(pair / ORB) - jnp.dot(known, known.T, precision=lax.Precision.HIGHEST)
        inner = lax.dot_general(orbitals.astype(jnp.float32), sampled.astype(jnp.float32), (((0,), (0,)), ((), ())), preferred_element_type=jnp.float32)
        columns = jnp.square(inner / ORB) - jnp.dot(factor, known.T, precision=lax.Precision.HIGHEST)
        lower = jnp.linalg.cholesky(block)
        fresh = jax.scipy.linalg.solve_triangular(lower, columns.T, lower=True).T
        factor = factor.at[:, section * PIV:(section + 1) * PIV].set(fresh)
        diagonal = diagonal - jnp.sum(fresh * fresh, axis=1)
        peaks.append(jnp.max(diagonal))
    return (factor, diagonal, jnp.stack(peaks))
```

```python
import functools

import jax
import jax.numpy as jnp
from jax import lax
from jax.experimental import pallas as pl
from jax.experimental.pallas import tpu as pltpu
from jax.sharding import Mesh
from jax.sharding import PartitionSpec as P

ORB = 1800
ALONG = ("x", "z", "core")
EVERYONE = ("x", "z", "core", "orb")
CHIPS = ("x", "z", "orb")
PAD = 512
HIGHEST = lax.Precision.HIGHEST


def nn(a, b, precision=None):
    return lax.dot_general(
        a, b, (((1,), (0,)), ((), ())), precision=precision, preferred_element_type=jnp.float32
    )


def nt(a, b, precision=None):
    return lax.dot_general(
        a, b, (((1,), (1,)), ((), ())), precision=precision, preferred_element_type=jnp.float32
    )


def tn(a, b, precision=None):
    return lax.dot_general(
        a, b, (((0,), (0,)), ((), ())), precision=precision, preferred_element_type=jnp.float32
    )


def pick_kernel(width, local_ref, orbitals_ref, out_ref, acc_ref):
    step = pl.program_id(0)

    @pl.when(step == 0)
    def _():
        acc_ref[...] = jnp.zeros_like(acc_ref)

    columns = local_ref.shape[1]
    spot = lax.broadcasted_iota(jnp.int32, (width, columns), 0) + step * width
    chosen = jnp.where(spot == local_ref[...], 1.0, 0.0).astype(jnp.bfloat16)
    acc_ref[...] += nn(orbitals_ref[...], chosen)

    @pl.when(step == pl.num_programs(0) - 1)
    def _():
        rows = acc_ref.shape[0]
        out_ref[0:rows, :] = acc_ref[...].astype(jnp.bfloat16)
        out_ref[rows:, :] = jnp.zeros((PAD - rows, columns), jnp.bfloat16)


def pick(orbitals, local, width=1024):
    rows, points = orbitals.shape
    columns = local.shape[1]
    return pl.pallas_call(
        functools.partial(pick_kernel, width),
        grid=(points // width,),
        in_specs=[
            pl.BlockSpec((1, columns), lambda i: (0, 0)),
            pl.BlockSpec((rows, width), lambda i: (0, i)),
        ],
        out_specs=pl.BlockSpec((PAD, columns), lambda i: (0, 0)),
        out_shape=jax.ShapeDtypeStruct((PAD, columns), jnp.bfloat16),
        scratch_shapes=[pltpu.VMEM((rows, columns), jnp.float32)],
        cost_estimate=pl.CostEstimate(
            flops=2 * rows * points * columns, bytes_accessed=2 * rows * points, transcendentals=0
        ),
        name="pick",
    )(local, orbitals)


def pair_kernel(where_ref, first_ref, second_ref, near_ref, far_ref, out_ref):
    rows = near_ref.shape[0]
    count = first_ref.shape[0]
    near = near_ref[...]
    far = far_ref[...]
    out_ref[0:count, :] = nn(first_ref[:, 0:rows], near) + nn(second_ref[:, 0:rows], far)
    near = near.astype(jnp.float32)
    far = far.astype(jnp.float32)
    total = jnp.sum(near * near + far * far, axis=0, keepdims=True)
    out_ref[count:, :] = jnp.broadcast_to(total, (8, total.shape[1]))


def pair(orbitals, start, first, far, second, width=512):
    rows = orbitals.shape[0]
    count = first.shape[0]
    points = far.shape[1]
    blocks = start // width
    return pl.pallas_call(
        pair_kernel,
        grid_spec=pltpu.PrefetchScalarGridSpec(
            num_scalar_prefetch=1,
            grid=(points // width,),
            in_specs=[
                pl.BlockSpec((count, PAD), lambda i, w: (0, 0)),
                pl.BlockSpec((count, PAD), lambda i, w: (0, 0)),
                pl.BlockSpec((rows, width), lambda i, w: (0, w[0] + i)),
                pl.BlockSpec((rows, width), lambda i, w: (0, i)),
            ],
            out_specs=pl.BlockSpec((count + 8, width), lambda i, w: (0, i)),
        ),
        out_shape=jax.ShapeDtypeStruct((count + 8, points), jnp.float32),
        cost_estimate=pl.CostEstimate(
            flops=4 * rows * points * count, bytes_accessed=8 * rows * points, transcendentals=0
        ),
        name="pair",
    )(blocks.reshape(1), first, second, orbitals, far)


def inverse_factor(block):
    size = block.shape[0]
    lane = lax.broadcasted_iota(jnp.int32, (8, 128), 1)
    sub = lax.broadcasted_iota(jnp.int32, (8, 128), 0)
    left = [block[8 * g : 8 * g + 8, :] for g in range(size // 8)]
    right = [jnp.where(lane == sub + 8 * g, 1.0, 0.0) for g in range(size // 8)]
    for j in range(size):
        g, r = divmod(j, 8)
        here = left[g]
        d = here[r : r + 1, j : j + 1]
        scale = 1.0 / d
        lead_left = here[r : r + 1, :] * scale
        lead_right = right[g][r : r + 1, :] * scale
        for k in range(g, size // 8):
            if k == g and r == 7:
                continue
            column = left[k][:, j : j + 1]
            if k == g:
                column = jnp.where(sub[:, 0:1] > r, column, 0.0)
            left[k] = left[k] - column * lead_left
            right[k] = right[k] - column * lead_right
    out = []
    for g in range(size // 8):
        own = jnp.sum(jnp.where(lane == sub + 8 * g, left[g], 0.0), axis=1, keepdims=True)
        out.append(right[g] * lax.rsqrt(own))
    return jnp.concatenate(out, axis=0)


def chain_kernel(steps, size, pivots_ref, inverse_ref, cross_ref, work_ref):
    for t in range(steps):
        for u in range(t, steps):
            total = jnp.zeros((size, size), jnp.float32)
            for y in range(pivots_ref.shape[0]):
                total = total + nt(
                    pivots_ref[y, size * t : size * t + size, :],
                    pivots_ref[y, size * u : size * u + size, :],
                )
            scaled = total / ORB
            work_ref[t, u] = jnp.zeros((size, 128), jnp.float32)
            work_ref[t, u, :, 0:size] = scaled * scaled
    slot = 0
    for s in range(steps):
        inverse = inverse_factor(work_ref[s, s])
        inverse_ref[s] = inverse
        crosses = []
        for t in range(s + 1, steps):
            cross = nn(inverse[:, 0:size], work_ref[s, t], HIGHEST)
            cross_ref[slot] = cross
            slot += 1
            crosses.append((t, cross))
        for t, left in crosses:
            for u, right in crosses:
                if u >= t:
                    work_ref[t, u] = work_ref[t, u] - tn(left, right, HIGHEST)[0:size, :]


def chain(pivot_rows, steps, size):
    pairs = steps * (steps - 1) // 2
    return pl.pallas_call(
        functools.partial(chain_kernel, steps, size),
        out_shape=(
            jax.ShapeDtypeStruct((steps, size, 128), jnp.float32),
            jax.ShapeDtypeStruct((pairs, size, 128), jnp.float32),
        ),
        scratch_shapes=[pltpu.VMEM((steps, steps, size, 128), jnp.float32)],
        cost_estimate=pl.CostEstimate(flops=10**10, bytes_accessed=4 * 10**6, transcendentals=0),
        name="chain",
    )(pivot_rows)


def solve_kernel(steps, size, half, base_ref, a_ref, b_ref, inverse_ref, cross_ref, factor_ref, diagonal_ref, peak_ref):
    step = pl.program_id(0)
    total = steps * size
    other = jnp.where(step < half, a_ref[...], b_ref[...])
    inner = (base_ref[...] + other) / ORB
    inner = inner * inner
    diagonal = inner[total : total + 1, :]
    done = []
    for s in range(steps):
        column = inner[size * s : size * s + size, :]
        for t in range(s):
            slot = sum(steps - 1 - k for k in range(t)) + (s - t - 1)
            column = column - tn(cross_ref[slot], done[t], HIGHEST)[0:size, :]
        fresh = nn(inverse_ref[s, :, 0:size], column, HIGHEST)
        done.append(fresh)
        factor_ref[size * s : size * s + size, :] = fresh
        diagonal = diagonal - jnp.sum(fresh * fresh, axis=0, keepdims=True)
        top = jnp.broadcast_to(jnp.max(diagonal, axis=1, keepdims=True), (1, 128))

        @pl.when(step == 0)
        def _(s=s, top=top):
            peak_ref[s : s + 1, :] = top

        @pl.when(step > 0)
        def _(s=s, top=top):
            peak_ref[s : s + 1, :] = jnp.maximum(peak_ref[s : s + 1, :], top)

    diagonal_ref[...] = diagonal


def solve(base, a, b, inverses, crosses, steps, size, width=512):
    rows, points = base.shape
    total = steps * size
    half = a.shape[1] // width
    return pl.pallas_call(
        functools.partial(solve_kernel, steps, size, half),
        grid=(points // width,),
        in_specs=[
            pl.BlockSpec((rows, width), lambda i: (0, i)),
            pl.BlockSpec((rows, width), lambda i: (0, jnp.minimum(i, half - 1))),
            pl.BlockSpec((rows, width), lambda i: (0, jnp.maximum(i - half, 0))),
            pl.BlockSpec(inverses.shape, lambda i: (0, 0, 0)),
            pl.BlockSpec(crosses.shape, lambda i: (0, 0, 0)),
        ],
        out_specs=(
            pl.BlockSpec((total, width), lambda i: (0, i)),
            pl.BlockSpec((1, width), lambda i: (0, i)),
            pl.BlockSpec((8, 128), lambda i: (0, 0)),
        ),
        out_shape=(
            jax.ShapeDtypeStruct((total, points), jnp.float32),
            jax.ShapeDtypeStruct((1, points), jnp.float32),
            jax.ShapeDtypeStruct((8, 128), jnp.float32),
        ),
        cost_estimate=pl.CostEstimate(flops=10**9, bytes_accessed=10**7, transcendentals=0),
        name="solve",
    )(base, a, b, inverses, crosses)


def ring(n, shift):
    return [(i, (i + shift) % n) for i in range(n)]


def everyone(x, axes, count):
    return lax.all_to_all(
        jnp.broadcast_to(x[None], (count, *x.shape)), axes, split_axis=0, concat_axis=0, tiled=True
    )


def after(x, *others):
    return lax.optimization_barrier((x, *others))[0]


def on_device(orbitals, pivots):
    rows, points = orbitals.shape
    n = lax.axis_size("orb")
    devices = lax.axis_size(ALONG)
    share = points // n
    half = share // 2
    steps, size = pivots.shape
    total = steps * size
    y = lax.axis_index("orb")
    here = lax.axis_index(ALONG) * points

    def chunk(owner, late):
        return lax.rem(owner + n, n) * share + late * half

    def piece(start):
        return lax.dynamic_slice(orbitals, (0, start), (rows, half))

    def send(x, shift):
        return lax.ppermute(x, "orb", ring(n, shift))

    relay_up = send(piece(chunk(y + 2, 0)), 1)
    relay_down = send(piece(chunk(y + 2, 1)), n - 1)

    mine = pick(orbitals, pivots.reshape(1, total) - here)
    mine = lax.all_to_all(
        mine.reshape(devices, PAD // devices, total), ALONG, split_axis=0, concat_axis=0, tiled=True
    )
    mine = jnp.sum(mine.astype(jnp.float32), axis=0).astype(jnp.bfloat16)
    column = everyone(mine, "orb", n)

    near_up = send(after(piece(chunk(y + 1, 1)), column), 1)
    near_down = send(after(piece(chunk(y - 1, 0)), column), n - 1)

    everything = everyone(column, ALONG, devices)
    spread = jnp.transpose(everything, (1, 3, 0, 2)).reshape(n, total, PAD)

    def of(owner):
        return lax.dynamic_index_in_dim(spread, lax.rem(owner + n, n), 0, keepdims=False)

    own, up, down = of(y), of(y + 1), of(y - 1)

    partial_up = pair(orbitals, chunk(y + 1, 0), own, relay_up, down)
    partial_down = pair(orbitals, chunk(y - 1, 1), own, relay_down, up)
    a = send(partial_up, 1)
    b = send(partial_down, n - 1)

    inverses, crosses = chain(spread, steps, size)
    base = jnp.concatenate(
        [
            pair(orbitals, chunk(y, 0), own, near_down, up),
            pair(orbitals, chunk(y, 1), own, near_up, down),
        ],
        axis=1,
    )
    factor, diagonal, peaks = solve(base, a, b, inverses, crosses, steps, size)
    peaks = jnp.maximum(peaks, lax.ppermute(peaks, "core", [(0, 1), (1, 0)]))
    peaks = everyone(peaks, CHIPS, lax.axis_size(CHIPS))
    peaks = jnp.max(peaks, axis=0)[0:steps, 0]
    return (factor.T, diagonal.reshape(share), peaks)


def solution(mesh):
    split = Mesh(
        mesh.devices.reshape(4, 4, 2, mesh.shape["orb"]), ("x", "z", "core", "orb")
    )
    return jax.shard_map(
        on_device,
        mesh=split,
        in_specs=(P("orb", ALONG), P()),
        out_specs=(P(EVERYONE, None), P(EVERYONE), P()),
        check_vma=False,
    )
```
